32 devices in a mesh: band: 4 (over z), sector: 8 (over y, x, core).
Axes of the slice: x: 2, y: 2, z: 4, core: 2. Of those that a mesh axis runs over, the one named last changes fastest.
Arguments:
- field: float32 [2, 640, 2, 2560], P(None, 'band', None, 'sector'), may hold values from -6 to 6
- depart: int32 [2, 640, 80], P(None, 'band', 'sector'), may hold values from -2 to 2
- interp_weight: bfloat16 [2, 640, 80, 64, 32], P(None, 'band', 'sector'), may hold values from -0.75 to 0.75
- legendre: float32 [640, 640, 1281], P('sector', 'band'), may hold values from -0.25 to 0.25
- damping: float32 [2], replicated, may hold values from 0.3 to 30
Outputs:
- new_field: float32 [2, 640, 2, 2560], P(None, 'band', None, 'sector')
The draws below stay inside these ranges and needn't reach their ends.
All inputs are finite; a program needn't handle non-finite values.
Results may differ from the reference program's by a relative error of at most 0.0003.
Values sent between devices are 32-bit elements; how exact they have to be, the bound alone decides.
No kernel may reach another device: no remote copies, remote signals or barrier semaphores. Data moves between devices by JAX's collectives and lax.ppermute only.
A program may use at most 192 MiB of HBM per device.

```python
import math
import jax
import jax.numpy as jnp
from jax import lax

NLON = 2560
M = 1280
TILE = 32
LEV = 2
NH = 640
MPAIR = 640


def set_ends(values, rng, least, high):
    place = [jax.random.randint(jax.random.fold_in(rng, axis), (), 0, length) for axis, length in enumerate(values.shape)]
    widest = values.shape.index(max(values.shape))
    next_to = place[:widest] + [(place[widest] + 1) % values.shape[widest]] + place[widest + 1:]
    return values.at[tuple(place)].set(least).at[tuple(next_to)].set(high)


def steps_of(key, shape, cuts, smallest, largest):
    level = 1.0
    for dim, parts in cuts:
        steps = jax.random.uniform(jax.random.fold_in(jax.random.fold_in(key, 6), dim), (parts,), jnp.float32, smallest / len(cuts), largest / len(cuts))
        level = level * jnp.repeat(jnp.exp(steps), shape[dim] // parts).reshape((-1,) + (1,) * (len(shape) - 1 - dim))
    return level


def normal_values(rng, dims, scale, most, cuts=(), kind=jnp.bfloat16):
    level = steps_of(rng, dims, cuts, -0.22, 0.18) if cuts else 1.0
    entries = jax.random.normal(rng, dims, jnp.float32) * scale * level
    return jnp.minimum(jnp.maximum(entries, -most), most).astype(kind)


def setup_inputs(seed: int = 0) -> dict:
    streams_of = jax.random.split(jax.random.key(seed), 6)
    field = normal_values(streams_of[0], (2, NH, LEV, NLON), 1.0, 6.0, ((1, 4), (3, 8)), jnp.float32)
    depart = set_ends(jax.random.randint(streams_of[1], (2, NH, NLON // TILE), -2, 3), jax.random.fold_in(streams_of[1], 1), -2, 2).astype(jnp.int32)
    interp_weight = normal_values(streams_of[2], (2, NH, NLON // TILE, 2 * TILE, TILE), (2 * TILE) ** -0.5, 0.75, ((1, 4), (2, 8)))
    legendre = normal_values(streams_of[3], (MPAIR, NH, M + 1), NH ** -0.5, 0.25, ((0, 8), (1, 4)), jnp.float32)
    damping = jnp.clip(jnp.exp(jax.random.uniform(streams_of[4], (LEV,), jnp.float32, math.log(0.3), math.log(30.0))), 0.3, 30.0)
    return {"field": field, "depart": depart, "interp_weight": interp_weight, "legendre": legendre, "damping": damping}


HIGHEST = lax.Precision.HIGHEST


def pair_masks(pair_index, m_count, row_count):
    column = jnp.arange(row_count, dtype=jnp.int32)[None, :]
    limit = (m_count - pair_index)[:, None]
    leading = column < limit
    lag_value = jnp.where(leading, column, column - limit)
    odd_rows = (lag_value % 2) == 1
    degree = jnp.where(leading, pair_index[:, None] + column, column - 1)
    return leading, odd_rows, degree


def analyse(wave, legendre, leading, odd_rows):
    stacked = jnp.stack([wave[0] + wave[1], wave[0] - wave[1]])
    product = jnp.einsum('svcpl,plk->svcpk', stacked, legendre, precision=HIGHEST)
    chosen = jnp.where(odd_rows, product[1], product[0])
    return jnp.where(leading, chosen[:, 0:2], chosen[:, 2:4])


def solve_modes(spectrum, damping_levels, degree, m_count):
    ratio = (degree * (degree + 1)).astype(jnp.float32) / float(m_count * m_count)
    return spectrum / (1.0 + damping_levels[:, None, None, None] * ratio[None, None])


def synthesise(spectrum, legendre, leading, odd_rows):
    lower = jnp.where(leading, spectrum, 0.0)
    upper = jnp.where(leading, 0.0, spectrum)
    northern = jnp.concatenate([lower, upper], axis=1)
    southern = jnp.where(odd_rows, -northern, northern)
    stacked = jnp.stack([northern, southern])
    return jnp.einsum('hvcpk,plk->hvcpl', stacked, legendre, precision=HIGHEST)


def reference(field, depart, interp_weight, legendre, damping):
    hemis, lat_count, level_count, lon_count = field.shape
    tile_width = interp_weight.shape[-1]
    tile_count = lon_count // tile_width
    pieces = field.reshape(hemis, lat_count, level_count, tile_count, tile_width)
    lead_tile = (jnp.arange(tile_count, dtype=jnp.int32)[None, None, :] + depart) % tile_count
    next_tile = (lead_tile + 1) % tile_count
    full_shape = (hemis, lat_count, level_count, tile_count, tile_width)
    lead_part = jnp.take_along_axis(pieces, jnp.broadcast_to(lead_tile[:, :, None, :, None], full_shape), axis=3)
    next_part = jnp.take_along_axis(pieces, jnp.broadcast_to(next_tile[:, :, None, :, None], full_shape), axis=3)
    window = jnp.concatenate([lead_part, next_part], axis=4)
    advected = jnp.einsum('hlvtj,hltji->hlvti', window, interp_weight.astype(jnp.float32), precision=HIGHEST)
    advected = advected.reshape(hemis, lat_count, level_count, lon_count)
    row_count = legendre.shape[2]
    m_count = row_count - 1
    pair_total = m_count // 2
    spectral = jnp.fft.rfft(advected, axis=-1) / lon_count
    lower_waves = spectral[..., :pair_total]
    upper_waves = spectral[..., pair_total:m_count][..., ::-1]
    stacked = jnp.stack([jnp.real(lower_waves), jnp.imag(lower_waves), jnp.real(upper_waves), jnp.imag(upper_waves)], axis=3)
    wave = jnp.transpose(stacked, (0, 2, 3, 4, 1)).astype(jnp.float32)
    pair_index = jnp.arange(pair_total, dtype=jnp.int32)
    leading, odd_rows, degree = pair_masks(pair_index, m_count, row_count)
    spectrum = analyse(wave, legendre, leading, odd_rows)
    solved = solve_modes(spectrum, damping, degree, m_count)
    synthesis = synthesise(solved, legendre, leading, odd_rows)
    lower_coef = synthesis[:, :, 0] + 1j * synthesis[:, :, 1]
    upper_coef = synthesis[:, :, 2] + 1j * synthesis[:, :, 3]
    padding = jnp.zeros((hemis, level_count, lon_count // 2 + 1 - m_count, lat_count), lower_coef.dtype)
    coefficients = jnp.concatenate([lower_coef, upper_coef[:, :, ::-1], padding], axis=2)
    coefficients = jnp.transpose(coefficients, (0, 3, 1, 2))
    return jnp.fft.irfft(coefficients, n=lon_count, axis=-1) * lon_count
```

```python
import functools
import math

import jax
import jax.numpy as jnp
import numpy as np
from jax import lax
from jax.experimental import pallas as pl
from jax.experimental.pallas import tpu as pltpu
from jax.sharding import PartitionSpec as P

REACH_BACK = 2
REACH_AHEAD = 3
CHUNKS = 2
LANES = 128
WIDE = 256
F32 = jnp.float32
BF16 = jnp.bfloat16


def params(*semantics):
    return pltpu.CompilerParams(dimension_semantics=semantics, vmem_limit_bytes=48 * 1024 * 1024)


def cost(flops, moved):
    return pl.CostEstimate(flops=int(flops), bytes_accessed=int(moved), transcendentals=0)


def split(x):
    high = x.astype(BF16)
    low = (x - high.astype(F32)).astype(BF16)
    return high, low


def split_np(x):
    high = np.asarray(x, np.float32).astype(jnp.bfloat16)
    low = (np.asarray(x, np.float64) - high.astype(np.float64)).astype(np.float32).astype(jnp.bfloat16)
    return high, low


def advect_kernel(field_ref, before_ref, after_ref, depart_ref, weight_ref, out_ref, extended, window, *, width, parts, share):
    tile = pl.program_id(1)
    levels, local = field_ref.shape[1], field_ref.shape[2]
    back, ahead = REACH_BACK * width, REACH_AHEAD * width

    @pl.when(tile == 0)
    def _():
        for v in range(levels):
            extended[v, 0:back] = before_ref[0, v]
            extended[v, back : back + local] = field_ref[0, v]
            extended[v, back + local : back + local + ahead] = after_ref[0, v]

    depart = depart_ref[0, 0]
    start = pl.multiple_of(tile * width, width)
    for v in range(levels):
        for half in range(0, 2 * width, 8):
            picked = None
            for step in range(2 * REACH_BACK + 1):
                rows = extended[v, pl.ds(start + step * width + half, 8), :]
                chosen = depart == (step - REACH_BACK)
                picked = rows if picked is None else jnp.where(chosen, rows, picked)
            window[v, half : half + 8] = picked
    columns = field_ref.shape[3]

    def body(block, totals):
        for j in range(8):
            row = block * 8 + j
            weight = weight_ref[0, 0, row].astype(F32)
            totals = tuple(
                totals[v] + window[v, pl.ds(row, 1), :] * weight for v in range(levels)
            )
        return totals

    zero = jnp.zeros((width, columns), F32)
    totals = lax.fori_loop(0, 2 * width // 8, body, (zero,) * levels)
    for v in range(levels):
        for part in range(parts):
            out_ref[v * parts + part, :, 0:share] = totals[v][:, part * share : (part + 1) * share]


def advect(field, depart, interp_weight, sectors):
    hemis, lats, levels, local = field.shape
    width = interp_weight.shape[-1]
    tiles = depart.shape[2]
    parts = sectors // (hemis * levels)
    share = lats // parts
    turned = jnp.transpose(field, (0, 2, 3, 1))
    up = [(i, (i + 1) % sectors) for i in range(sectors)]
    down = [(j, i) for i, j in up]
    before = lax.ppermute(turned[:, :, local - REACH_BACK * width :], "sector", up)
    after = lax.ppermute(turned[:, :, : REACH_AHEAD * width], "sector", down)
    weights = jnp.transpose(interp_weight, (0, 2, 3, 4, 1))
    offsets = jnp.transpose(depart, (0, 2, 1))[:, :, None, :]
    return pl.pallas_call(
        functools.partial(advect_kernel, width=width, parts=parts, share=share),
        grid=(hemis, tiles),
        in_specs=[
            pl.BlockSpec((1, levels, local, lats), lambda h, t: (h, 0, 0, 0)),
            pl.BlockSpec((1, levels, REACH_BACK * width, lats), lambda h, t: (h, 0, 0, 0)),
            pl.BlockSpec((1, levels, REACH_AHEAD * width, lats), lambda h, t: (h, 0, 0, 0)),
            pl.BlockSpec((1, 1, 1, lats), lambda h, t: (h, t, 0, 0)),
            pl.BlockSpec((1, 1, 2 * width, width, lats), lambda h, t: (h, t, 0, 0, 0)),
        ],
        out_specs=pl.BlockSpec((levels * parts, width, LANES), lambda h, t: (h, t, 0)),
        out_shape=jax.ShapeDtypeStruct((sectors, local, LANES), F32),
        scratch_shapes=[
            pltpu.VMEM((levels, local + (REACH_BACK + REACH_AHEAD) * width, lats), F32),
            pltpu.VMEM((levels, 2 * width, lats), F32),
        ],
        compiler_params=params("arbitrary", "arbitrary"),
        cost_estimate=cost(4 * hemis * tiles * levels * 2 * width * width * lats * 4, interp_weight.size * 3),
        name="advect",
    )(turned, before, after, offsets, weights)


def fourier_tables(lon_count, radix):
    inner = lon_count // radix
    waves = lon_count // 2
    slots = waves // 2 // radix
    index = np.arange(slots)
    direct = index
    mirror = waves // radix - 1 - index
    rows = []
    for kind in range(2):
        for component in range(4):
            degree = direct if component < 2 else mirror
            source = degree if kind == 0 else inner - 1 - degree
            angle = 2.0 * np.pi * ((source[:, None] * np.arange(inner)[None, :]) % inner) / inner
            if component % 2 == 0:
                row = np.concatenate([np.cos(angle), np.sin(angle)], axis=1)
            else:
                sign = 1.0 if kind == 0 else -1.0
                row = sign * np.concatenate([-np.sin(angle), np.cos(angle)], axis=1)
            rows.append(row)
    matrix = np.concatenate(rows, axis=0)
    order = np.arange(radix // 2 + 1)[:, None] * np.arange(inner)[None, :]
    angle = 2.0 * np.pi * (order % lon_count) / lon_count
    twiddle = np.stack([np.cos(angle), -np.sin(angle)], axis=1).astype(np.float32)
    return matrix, twiddle


def scaled(x, factor):
    if abs(factor - 1.0) < 1e-12:
        return x
    if abs(factor + 1.0) < 1e-12:
        return -x
    return x * np.float32(factor)


def combine(terms):
    total = None
    for factor, x in terms:
        if abs(factor) < 1e-12:
            continue
        total = scaled(x, factor) if total is None else total + scaled(x, factor)
    return total


def products(high_ref, low_ref, rows, depth, x):
    x_high, x_low = split(x)
    both = jnp.concatenate([x_high, x_low], axis=1)
    first = jnp.dot(high_ref[0:rows, 0:depth], both, preferred_element_type=F32)
    second = jnp.dot(low_ref[0:rows, 0:depth], x_high, preferred_element_type=F32)
    return first[:, 0:LANES] + first[:, LANES:] + second


def places(a, radix):
    residues = [a] if a in (0, radix // 2) else [a, radix - a]
    result = []
    for residue in residues:
        for component in range(4):
            first = residue if component < 2 else radix - 1 - residue
            result.append(first * 4 + component)
    return result


def forward_kernel(x_ref, high_ref, low_ref, twiddle_ref, out_ref, *, radix):
    inner = x_ref.shape[0] // radix
    slots = out_ref.shape[0] // (4 * radix)
    x = [x_ref[s * inner : (s + 1) * inner] for s in range(radix)]
    middle = radix // 2
    even = {s: x[s] + x[radix - s] for s in range(1, middle)}
    odd = {s: x[s] - x[radix - s] for s in range(1, middle)}
    for a in range(middle + 1):
        angle = [2.0 * math.pi * ((a * s) % radix) / radix for s in range(radix)]
        real = combine([(1.0, x[0]), (math.cos(angle[middle]), x[middle])] + [(math.cos(angle[s]), even[s]) for s in even])
        imag = combine([(-math.sin(angle[s]), odd[s]) for s in odd])
        where = places(a, radix)
        if a == 0:
            result = products(high_ref, low_ref, len(where) * slots, inner, real)
        else:
            cos, sin = twiddle_ref[a, 0], twiddle_ref[a, 1]
            turned_real = cos * real if imag is None else cos * real - sin * imag
            turned_imag = sin * real if imag is None else sin * real + cos * imag
            turned = jnp.concatenate([turned_real, turned_imag], axis=0)
            result = products(high_ref, low_ref, len(where) * slots, 2 * inner, turned)
        for n, first in enumerate(where):
            out_ref[pl.ds(first, slots, stride=4 * radix), :] = result[n * slots : (n + 1) * slots]


def inverse_kernel(z_ref, high_ref, low_ref, twiddle_ref, out_ref, *, radix):
    inner = out_ref.shape[0] // radix
    slots = z_ref.shape[0] // (4 * radix)
    middle = radix // 2
    reals, imags = [], []
    for a in range(middle + 1):
        where = places(a, radix)
        pieces = [z_ref[pl.ds(first, slots, stride=4 * radix), :] for first in where]
        if a == 0:
            row = lax.broadcasted_iota(jnp.int32, pieces[0].shape, 0)
            pieces[0] = jnp.where(row == 0, 0.5 * pieces[0], pieces[0])
        column = jnp.concatenate(pieces, axis=0)
        depth = len(where) * slots
        if a == 0:
            reals.append(products(high_ref, low_ref, inner, depth, column))
            imags.append(None)
            continue
        result = products(high_ref, low_ref, 2 * inner, depth, column)
        real, imag = result[0:inner], result[inner:]
        cos, sin = twiddle_ref[a, 0], twiddle_ref[a, 1]
        reals.append(cos * real + sin * imag)
        imags.append(None if a == middle else cos * imag - sin * real)
    for s in range(middle + 1):
        angle = [2.0 * math.pi * ((a * s) % radix) / radix for a in range(middle + 1)]
        even = combine([(math.cos(angle[a]), reals[a]) for a in range(middle + 1)])
        odd = combine([(-math.sin(angle[a]), imags[a]) for a in range(1, middle)])
        if s == 0 or s == middle:
            out_ref[s * inner : (s + 1) * inner] = even
        else:
            out_ref[s * inner : (s + 1) * inner] = even + odd
            other = radix - s
            out_ref[other * inner : (other + 1) * inner] = even - odd


def transform(kernel, x, high, low, twiddle, radix, name):
    rows = x.shape[0]
    return pl.pallas_call(
        functools.partial(kernel, radix=radix),
        out_shape=jax.ShapeDtypeStruct((rows, LANES), F32),
        compiler_params=pltpu.CompilerParams(vmem_limit_bytes=48 * 1024 * 1024),
        cost_estimate=cost(3 * 2 * high.size * LANES * radix, 4 * rows * LANES * 4),
        name=name,
    )(x, high, low, twiddle)


def row_masks(pair, waves, shape, first):
    column = first + lax.broadcasted_iota(jnp.int32, shape, 1)
    limit = waves - pair
    leading = column < limit
    lag = jnp.where(leading, column, column - limit)
    odd = (lag & 1) == 1
    return column, leading, odd


def ranges(count):
    edges = list(range(0, count - count % WIDE, WIDE)) + [count]
    return list(zip(edges[:-1], edges[1:]))


def gather_lats(z_ref, hemi, level, levels, parts, share, start):
    rows = [z_ref[(hemi * levels + level) * parts + part, pl.ds(start, 8), 0:share] for part in range(parts)]
    return jnp.concatenate(rows, axis=1)


def analyse_kernel(place_ref, z_ref, legendre_ref, out_ref, *, levels, parts, share):
    step = place_ref[0] + pl.program_id(0)
    count = legendre_ref.shape[2]
    waves = count - 1
    start = pl.multiple_of(step * 8, 8)
    sums, differences = [], []
    for v in range(levels):
        north = gather_lats(z_ref, 0, v, levels, parts, share, start)
        south = gather_lats(z_ref, 1, v, levels, parts, share, start)
        sums.append(north + south)
        differences.append(north - south)
    stacks = []
    for which in range(2):
        low, high = which * 4, which * 4 + 4
        wave = jnp.concatenate([x[low:high] for x in sums + differences], axis=0)
        wave_high, wave_low = split(wave)
        stacks.append((jnp.concatenate([wave_high, wave_low], axis=0), wave_high))
    for first, last in ranges(count):
        picked = []
        for which in range(2):
            both, wave_high = stacks[which]
            rows = both.shape[0] // 2
            high, low = split(legendre_ref[which, :, first:last])
            product = jnp.dot(both, high, preferred_element_type=F32)
            product = product[0:rows] + product[rows:] + jnp.dot(wave_high, low, preferred_element_type=F32)
            pair = place_ref[1] + 2 * step + which
            shape = (rows // 2, last - first)
            _, leading, odd = row_masks(pair, waves, shape, first)
            chosen = jnp.where(odd, product[rows // 2 :], product[0 : rows // 2])
            if which == 0:
                picked.append(jnp.where(leading, chosen, jnp.roll(chosen, -2, axis=0)))
            else:
                picked.append(jnp.where(leading, jnp.roll(chosen, 2, axis=0), chosen))
        component = lax.broadcasted_iota(jnp.int32, picked[0].shape, 0) % 4
        out_ref[0, :, first:last] = jnp.where(component < 2, picked[0], picked[1])


def analyse(place, z, legendre, steps, levels):
    pairs, lats, count = legendre.shape
    parts = z.shape[0] // (2 * levels)
    share = lats // parts
    return pl.pallas_call(
        functools.partial(analyse_kernel, levels=levels, parts=parts, share=share),
        grid_spec=pltpu.PrefetchScalarGridSpec(
            num_scalar_prefetch=1,
            grid=(steps,),
            in_specs=[
                pl.BlockSpec(z.shape, lambda i, place: (0, 0, 0)),
                pl.BlockSpec((2, lats, count), lambda i, place: (place[0] + i, 0, 0)),
            ],
            out_specs=pl.BlockSpec((1, 4 * levels, count), lambda i, place: (i, 0, 0)),
        ),
        out_shape=jax.ShapeDtypeStruct((steps, 4 * levels, count), F32),
        compiler_params=params("arbitrary"),
        cost_estimate=cost(16 * 2 * steps * lats * count * 20, 2 * steps * lats * count * 4),
        name="analyse",
    )(place, z, legendre)


def synthesise_kernel(place_ref, damping_ref, spectrum_ref, legendre_ref, *rest, levels, parts, share):
    out_ref = rest[-1]
    step = place_ref[0] + pl.program_id(0)
    count = legendre_ref.shape[2]
    waves = count - 1
    totals = [None, None]
    for first, last in ranges(count):
        spectrum = spectrum_ref[0, :, first:last]
        row = lax.broadcasted_iota(jnp.int32, spectrum.shape, 0)
        component = row % 4
        damping = jnp.full(spectrum.shape, damping_ref[levels - 1])
        for v in range(levels - 1):
            damping = jnp.where(row < 4 * (v + 1), damping_ref[v], damping) if v == 0 else damping
        for which in range(2):
            pair = place_ref[1] + 2 * step + which
            column, leading, odd = row_masks(pair, waves, spectrum.shape, first)
            degree = jnp.where(leading, pair + column, column - 1)
            ratio = (degree * (degree + 1)).astype(F32) / float(waves * waves)
            solved = spectrum / (1.0 + damping * ratio)
            if which == 0:
                doubled = jnp.where(component < 2, solved, jnp.roll(solved, 2, axis=0))
            else:
                doubled = jnp.where(component < 2, jnp.roll(solved, -2, axis=0), solved)
            keep = jnp.logical_xor(component >= 2, leading)
            north = jnp.where(keep, doubled, 0.0)
            south = jnp.where(odd, -north, north)
            high, low = split(jnp.concatenate([north, south], axis=0))
            both = jnp.concatenate([high, low], axis=0)
            legendre_high, legendre_low = split(legendre_ref[which, :, first:last])
            contract = (((1,), (1,)), ((), ()))
            one = lax.dot_general(legendre_high, both, contract, preferred_element_type=F32)
            two = lax.dot_general(legendre_low, both, contract, preferred_element_type=F32)
            total = one + two
            totals[which] = total if totals[which] is None else totals[which] + total
    rows = 4 * levels * 2
    waves_of = []
    for which in range(2):
        turned = jnp.transpose(totals[which], (1, 0))
        waves_of.append(turned[0:rows] + turned[rows:])
    for hemi in range(2):
        for v in range(levels):
            low = (hemi * levels + v) * 4
            block = jnp.concatenate([w[low : low + 4] for w in waves_of], axis=0)
            for part in range(parts):
                out_ref[(hemi * levels + v) * parts + part, :, 0:share] = block[:, part * share : (part + 1) * share]


def synthesise(place, damping, spectrum, legendre, previous, sectors):
    pairs, lats, count = legendre.shape
    levels = damping.shape[0]
    steps = spectrum.shape[0]
    parts = sectors // (2 * levels)
    share = lats // parts
    arguments = [place, damping, spectrum, legendre]
    in_specs = [
        pl.BlockSpec(memory_space=pltpu.SMEM),
        pl.BlockSpec((1, 4 * levels, count), lambda i, place: (i, 0, 0)),
        pl.BlockSpec((2, lats, count), lambda i, place: (place[0] + i, 0, 0)),
    ]
    aliases = {}
    if previous is not None:
        arguments.append(previous)
        in_specs.append(pl.BlockSpec(memory_space=pl.ANY))
        aliases = {4: 0}
    return pl.pallas_call(
        functools.partial(synthesise_kernel, levels=levels, parts=parts, share=share),
        grid_spec=pltpu.PrefetchScalarGridSpec(
            num_scalar_prefetch=1,
            grid=(steps,),
            in_specs=in_specs,
            out_specs=pl.BlockSpec((sectors, 8, LANES), lambda i, place: (0, place[0] + i, 0)),
        ),
        out_shape=jax.ShapeDtypeStruct((sectors, 4 * pairs, LANES), F32),
        input_output_aliases=aliases,
        compiler_params=params("arbitrary"),
        cost_estimate=cost(16 * 2 * steps * lats * count * 20, 2 * steps * lats * count * 4),
        name="synthesise",
    )(*arguments)


def solve(z, legendre, damping, sectors):
    pairs = legendre.shape[0]
    levels = damping.shape[0]
    bands = lax.axis_size("band")
    bit = lax.axis_index("band") % 2
    pair_start = lax.axis_index("sector") * pairs
    steps = pairs // (2 * 2 * CHUNKS)
    half = pairs // 4

    def place(side, chunk):
        return jnp.stack([side * half + chunk * steps, pair_start]).astype(jnp.int32)

    def swap(x, mask):
        return lax.ppermute(x, "band", [(i, i ^ mask) for i in range(bands)])

    def after(value, earlier):
        return value if earlier is None else lax.optimization_barrier((value, earlier))[0]

    masks = [1 << n for n in range(1, bands.bit_length()) if 1 << n < bands]
    sums, arrived, previous = [], [], None
    for c in range(CHUNKS):
        away = analyse(after(place(1 - bit, c), previous), z, legendre, steps, levels)
        kept = analyse(after(place(bit, c), away), z, legendre, steps, levels)
        previous = kept + swap(away, 1)
        sums.append(previous)
        arrived.append(swap(previous, masks[0]) if masks else jnp.zeros_like(previous))
    result = None
    for c in range(CHUNKS):
        total = sums[c] + after(arrived[c], sums[-1] if result is None else result)
        for mask in masks[1:]:
            total = total + swap(total, mask)
        other = swap(total, 1)
        result = synthesise(place(bit, c), damping, total, legendre, result, sectors)
        result = synthesise(place(1 - bit, c), damping, other, legendre, result, sectors)
    return result


def local(field, depart, interp_weight, legendre, damping):
    sectors = lax.axis_size("sector")
    hemis, lats, levels, local_lon = field.shape
    pairs = legendre.shape[0]
    lon_count = sectors * local_lon
    radix = math.gcd(sectors, pairs)
    matrix, twiddle = fourier_tables(lon_count, radix)
    forward_high, forward_low = split_np(matrix / lon_count)
    inverse_high, inverse_low = split_np(2.0 * matrix.T)
    twiddle = jnp.broadcast_to(jnp.asarray(twiddle)[..., None], twiddle.shape + (LANES,))

    def exchange(x, rows):
        return lax.all_to_all(x.reshape(sectors, rows, LANES), "sector", split_axis=0, concat_axis=0, tiled=True)

    advected = advect(field, depart, interp_weight, sectors)
    columns = exchange(advected, local_lon)
    fourier = transform(forward_kernel, columns.reshape(-1, LANES), forward_high, forward_low, twiddle, radix, "forward")
    z = exchange(fourier, 4 * pairs)
    synthesis = solve(z, legendre, damping, sectors)
    returned = exchange(synthesis, 4 * pairs)
    gridded = transform(inverse_kernel, returned.reshape(-1, LANES), inverse_high, inverse_low, twiddle, radix, "inverse")
    final = exchange(gridded, local_lon)
    parts = sectors // (hemis * levels)
    share = lats // parts
    final = final[:, :, :share].reshape(hemis, levels, parts, local_lon, share)
    return jnp.transpose(final, (0, 2, 4, 1, 3)).reshape(hemis, lats, levels, local_lon)


def solution(mesh):
    return jax.shard_map(
        local,
        mesh=mesh,
        in_specs=(
            P(None, "band", None, "sector"),
            P(None, "band", "sector"),
            P(None, "band", "sector", None, None),
            P("sector", "band", None),
            P(),
        ),
        out_specs=P(None, "band", None, "sector"),
        check_vma=False,
    )
```

```python
import functools
import math

import jax
import jax.numpy as jnp
import numpy as np
from jax import lax
from jax.experimental import pallas as pl
from jax.experimental.pallas import tpu as pltpu
from jax.sharding import PartitionSpec as P


REACH_BACK = 2
REACH_AHEAD = 3
CHUNKS = 4
SPLITS = 2
INNER = 5
LANES = 128
UNIT = 64
RADIX = 16
DEPTH = 6
WEIGHT = 2
WIDE = 256
F32 = jnp.float32
BF16 = jnp.bfloat16


def params(*semantics):
    return pltpu.CompilerParams(dimension_semantics=semantics, vmem_limit_bytes=48 * 1024 * 1024)


def cost(flops, moved):
    return pl.CostEstimate(flops=int(flops), bytes_accessed=int(moved), transcendentals=0)


def split(x):
    high = x.astype(BF16)
    low = (x - high.astype(F32)).astype(BF16)
    return high, low


def split_np(x):
    high = np.asarray(x, np.float32).astype(jnp.bfloat16)
    low = (np.asarray(x, np.float64) - high.astype(np.float64)).astype(np.float32).astype(jnp.bfloat16)
    return high, low


def stream(step, steps, depth, copies):
    ahead = depth - 1

    @pl.when(step == 0)
    def _():
        for early in range(min(ahead, steps)):
            for copy in copies(early, early):
                copy.start()

    @pl.when(step + ahead < steps)
    def _():
        for copy in copies(step + ahead, lax.rem(step + ahead, depth)):
            copy.start()

    slot = lax.rem(step, depth)
    for copy in copies(step, slot):
        copy.wait()
    return slot


def piece_widths(share):
    return [w for w in (64, 32, 16) if share & w]


def packable(share, rows, lanes=LANES):
    return share < lanes and share % 16 == 0 and rows % UNIT == 0


def packed_rows(rows, share):
    return rows * share // LANES


def pack(x, share):
    rows, offset, blocks = x.shape[0], 0, []
    for w in piece_widths(share):
        folds = LANES // w
        h = rows // folds
        blocks.append(jnp.concatenate([x[b * h : (b + 1) * h, offset : offset + w] for b in range(folds)], axis=1))
        offset += w
    return jnp.concatenate(blocks, axis=0)


def unpack(y, share):
    rows = y.shape[0] * LANES // share
    first, columns = 0, []
    for w in piece_widths(share):
        folds = LANES // w
        h = rows // folds
        block = y[first : first + h]
        columns.append(jnp.concatenate([block[:, b * w : (b + 1) * w] for b in range(folds)], axis=0))
        first += h
    columns.append(jnp.zeros((rows, LANES - share), y.dtype))
    return jnp.concatenate(columns, axis=1)


def advect_kernel(groups_ref, *refs, width, parts, share, group, count, packed, halo):
    if halo:
        field_ref, before_ref, after_ref, depart_ref, weight_ref, _, out_ref, extended, window, weights, sems = refs
    else:
        field_ref, depart_ref, weight_ref, out_ref, extended, window, weights, sems = refs
    hemi, place = pl.program_id(0), pl.program_id(1)
    levels, local, columns = field_ref.shape[1], field_ref.shape[2], field_ref.shape[3]
    back, ahead = REACH_BACK * width, REACH_AHEAD * width

    @pl.when(place == 0)
    def _():
        for v in range(levels):
            extended[v, back : back + local] = field_ref[0, v]
            if halo:
                extended[v, 0:back] = before_ref[0, v]
                extended[v, back + local : back + local + ahead] = after_ref[0, v]

    def copies(step, slot):
        tiles = groups_ref[lax.rem(step, count)] * group
        source = lax.div(step, count)
        return [
            pltpu.make_async_copy(weight_ref.at[source, tiles + n], weights.at[slot, n], sems.at[slot, n])
            for n in range(group)
        ]

    slot = stream(hemi * count + place, 2 * count, DEPTH, copies)
    results = [[] for _ in range(levels)]
    for n in range(group):
        tile = groups_ref[place] * group + n
        depart = depart_ref[0, n]
        start = pl.multiple_of(tile * width, width)
        for v in range(levels):
            for half in range(0, 2 * width, 8):
                picked = None
                for step in range(2 * REACH_BACK + 1):
                    rows = extended[v, pl.ds(start + step * width + half, 8), :]
                    chosen = depart == (step - REACH_BACK)
                    picked = rows if picked is None else jnp.where(chosen, rows, picked)
                window[v, half : half + 8] = picked

        def body(block, totals):
            for j in range(8):
                row = block * 8 + j
                weight = weights[slot, n, row].astype(F32)
                totals = tuple(totals[v] + window[v, pl.ds(row, 1), :] * weight for v in range(levels))
            return totals

        zero = jnp.zeros((width, columns), F32)
        totals = lax.fori_loop(0, 2 * width // 8, body, (zero,) * levels)
        for v in range(levels):
            results[v].append(totals[v])
    for v in range(levels):
        value = jnp.concatenate(results[v], axis=0)
        for part in range(parts):
            mine = value[:, part * share : (part + 1) * share]
            if packed:
                out_ref[v * parts + part] = pack(mine, share)
            else:
                out_ref[v * parts + part, :, 0:share] = mine


def advect(field, depart, interp_weight, sectors):
    hemis, lats, levels, local = field.shape
    width = interp_weight.shape[-1]
    tiles = depart.shape[2]
    parts = sectors // (hemis * levels)
    share = lats // parts
    packed = packable(share, local) and UNIT % width == 0
    group = UNIT // width if packed else 1
    rows = packed_rows(group * width, share) if packed else width
    turned = jnp.transpose(field, (0, 2, 3, 1))
    up = [(i, (i + 1) % sectors) for i in range(sectors)]
    down = [(j, i) for i, j in up]
    before = lax.ppermute(turned[:, :, local - REACH_BACK * width :], "sector", up)
    after = lax.ppermute(turned[:, :, : REACH_AHEAD * width], "sector", down)
    weights = jnp.transpose(interp_weight, (0, 2, 3, 4, 1))
    offsets = jnp.transpose(depart, (0, 2, 1))[:, :, None, :]
    every = list(range(tiles // group))
    inner = [g for g in every if g * group >= REACH_BACK and (g + 1) * group - 1 + REACH_AHEAD < tiles]
    outer = [g for g in every if g not in inner]

    def call(groups, halo, previous):
        count = len(groups)
        field_specs = [pl.BlockSpec((1, levels, local, lats), lambda h, g, groups: (h, 0, 0, 0))]
        operands = [jnp.asarray(groups, jnp.int32), turned]
        if halo:
            for side in (before, after):
                field_specs.append(pl.BlockSpec((1,) + side.shape[1:], lambda h, g, groups: (h, 0, 0, 0)))
                operands.append(side)
        operands += [offsets, weights]
        in_specs = field_specs + [
            pl.BlockSpec((1, group, 1, lats), lambda h, g, groups: (h, groups[g], 0, 0)),
            pl.BlockSpec(memory_space=pl.ANY),
        ]
        aliases = {}
        if halo:
            operands.append(previous)
            in_specs.append(pl.BlockSpec(memory_space=pl.ANY))
            aliases = {len(operands) - 1: 0}
        return pl.pallas_call(
            functools.partial(advect_kernel, width=width, parts=parts, share=share, group=group, count=count, packed=packed, halo=halo),
            grid_spec=pltpu.PrefetchScalarGridSpec(
                num_scalar_prefetch=1,
                grid=(hemis, count),
                in_specs=in_specs,
                out_specs=pl.BlockSpec((levels * parts, rows, LANES), lambda h, g, groups: (h, groups[g], 0)),
                scratch_shapes=[
                    pltpu.VMEM((levels, local + (REACH_BACK + REACH_AHEAD) * width, lats), F32),
                    pltpu.VMEM((levels, 2 * width, lats), F32),
                    pltpu.VMEM((DEPTH, group, 2 * width, width, lats), BF16),
                    pltpu.SemaphoreType.DMA((DEPTH, group)),
                ],
            ),
            out_shape=jax.ShapeDtypeStruct((sectors, rows * len(every), LANES), F32),
            input_output_aliases=aliases,
            compiler_params=params("arbitrary", "arbitrary"),
            cost_estimate=cost(4 * hemis * count * group * levels * 2 * width * width * lats * 4, interp_weight.size * 3 * count // len(every)),
            name="advect_edge" if halo else "advect_inner",
        )(*operands)

    if inner:
        result = call(inner, False, None)
    else:
        result = jnp.zeros((sectors, rows * len(every), LANES), F32)
    return call(outer, True, result), packed, share


def fourier_tables(lon_count, radix):
    inner = lon_count // radix
    waves = lon_count // 2
    slots = waves // 2 // radix
    index = np.arange(slots)
    direct = index
    mirror = waves // radix - 1 - index
    rows = []
    for kind in range(2):
        for component in range(4):
            degree = direct if component < 2 else mirror
            source = degree if kind == 0 else inner - 1 - degree
            angle = 2.0 * np.pi * ((source[:, None] * np.arange(inner)[None, :]) % inner) / inner
            if component % 2 == 0:
                row = np.concatenate([np.cos(angle), np.sin(angle)], axis=1)
            else:
                sign = 1.0 if kind == 0 else -1.0
                row = sign * np.concatenate([-np.sin(angle), np.cos(angle)], axis=1)
            rows.append(row)
    matrix = np.concatenate(rows, axis=0)
    order = np.arange(radix // 2 + 1)[:, None] * np.arange(inner)[None, :]
    angle = 2.0 * np.pi * (order % lon_count) / lon_count
    twiddle = np.stack([np.cos(angle), -np.sin(angle)], axis=1).astype(np.float32)
    return matrix, twiddle


def scaled(x, factor):
    if abs(factor - 1.0) < 1e-12:
        return x
    if abs(factor + 1.0) < 1e-12:
        return -x
    return x * np.float32(factor)


def combine(terms):
    total = None
    for factor, x in terms:
        if abs(factor) < 1e-12:
            continue
        total = scaled(x, factor) if total is None else total + scaled(x, factor)
    return total


def products(high_ref, low_ref, rows, depth, x):
    x_high, x_low = split(x)
    both = jnp.concatenate([x_high, x_low], axis=1)
    first = jnp.dot(high_ref[0:rows, 0:depth], both, preferred_element_type=F32)
    second = jnp.dot(low_ref[0:rows, 0:depth], x_high, preferred_element_type=F32)
    return first[:, 0:LANES] + first[:, LANES:] + second


def places(a, radix):
    residues = [a] if a in (0, radix // 2) else [a, radix - a]
    result = []
    for residue in residues:
        for component in range(4):
            first = residue if component < 2 else radix - 1 - residue
            result.append(first * 4 + component)
    return result


def chunk_rows(rows, sectors):
    n = rows // (sectors * 2 * SPLITS)
    return [(block * n, block * n * SPLITS, n) for block in range(sectors * 2)]


def forward_kernel(x_ref, high_ref, low_ref, twiddle_ref, *refs, radix, share, rows, sectors):
    outs, scratch = refs[:SPLITS], refs[SPLITS:]
    inner = rows // radix
    slots = rows // (4 * radix)
    out_ref = scratch[0]
    if len(scratch) > 1:
        plain = scratch[1]
        short = packed_rows(UNIT, share)
        for unit in range(rows // UNIT):
            plain[unit * UNIT : (unit + 1) * UNIT] = unpack(x_ref[unit * short : (unit + 1) * short], share)
    else:
        plain = x_ref
    x = [plain[s * inner : (s + 1) * inner] for s in range(radix)]
    middle = radix // 2
    even = {s: x[s] + x[radix - s] for s in range(1, middle)}
    odd = {s: x[s] - x[radix - s] for s in range(1, middle)}
    for a in range(middle + 1):
        angle = [2.0 * math.pi * ((a * s) % radix) / radix for s in range(radix)]
        real = combine([(1.0, x[0]), (math.cos(angle[middle]), x[middle])] + [(math.cos(angle[s]), even[s]) for s in even])
        imag = combine([(-math.sin(angle[s]), odd[s]) for s in odd])
        where = places(a, radix)
        if a == 0:
            result = products(high_ref, low_ref, len(where) * slots, inner, real)
        else:
            cos, sin = twiddle_ref[a, 0], twiddle_ref[a, 1]
            turned_real = cos * real if imag is None else cos * real - sin * imag
            turned_imag = sin * real if imag is None else sin * real + cos * imag
            turned = jnp.concatenate([turned_real, turned_imag], axis=0)
            result = products(high_ref, low_ref, len(where) * slots, 2 * inner, turned)
        for n, first in enumerate(where):
            out_ref[pl.ds(first, slots, stride=4 * radix), :] = result[n * slots : (n + 1) * slots]
    for target, source, n in chunk_rows(rows, sectors):
        for c in range(SPLITS):
            outs[c][target : target + n] = out_ref[source + c * n : source + (c + 1) * n]


def inverse_kernel(*refs, radix, share, rows, sectors):
    ins, (high_ref, low_ref, twiddle_ref, final_ref, z_ref, *scratch) = refs[:SPLITS], refs[SPLITS:]
    out_ref = scratch[0] if scratch else final_ref
    inner = rows // radix
    slots = rows // (4 * radix)
    for source, target, n in chunk_rows(rows, sectors):
        for c in range(SPLITS):
            z_ref[target + c * n : target + (c + 1) * n] = ins[c][source : source + n]
    middle = radix // 2
    reals, imags = [], []
    for a in range(middle + 1):
        where = places(a, radix)
        pieces = [z_ref[pl.ds(first, slots, stride=4 * radix), :] for first in where]
        if a == 0:
            row = lax.broadcasted_iota(jnp.int32, pieces[0].shape, 0)
            pieces[0] = jnp.where(row == 0, 0.5 * pieces[0], pieces[0])
        column = jnp.concatenate(pieces, axis=0)
        depth = len(where) * slots
        if a == 0:
            reals.append(products(high_ref, low_ref, inner, depth, column))
            imags.append(None)
            continue
        result = products(high_ref, low_ref, 2 * inner, depth, column)
        real, imag = result[0:inner], result[inner:]
        cos, sin = twiddle_ref[a, 0], twiddle_ref[a, 1]
        reals.append(cos * real + sin * imag)
        imags.append(None if a == middle else cos * imag - sin * real)
    for s in range(middle + 1):
        angle = [2.0 * math.pi * ((a * s) % radix) / radix for a in range(middle + 1)]
        even = combine([(math.cos(angle[a]), reals[a]) for a in range(middle + 1)])
        odd = combine([(-math.sin(angle[a]), imags[a]) for a in range(1, middle)])
        if s == 0 or s == middle:
            out_ref[s * inner : (s + 1) * inner] = even
        else:
            out_ref[s * inner : (s + 1) * inner] = even + odd
            other = radix - s
            out_ref[other * inner : (other + 1) * inner] = even - odd
    if scratch:
        short = packed_rows(UNIT, share)
        for unit in range(rows // UNIT):
            final_ref[unit * short : (unit + 1) * short] = pack(out_ref[unit * UNIT : (unit + 1) * UNIT], share)


def finish_kernel(x_ref, out_ref, plain, *, levels, parts, share):
    short = packed_rows(UNIT, share)
    for v in range(levels):
        for part in range(parts):
            for unit in range(plain.shape[0] // UNIT):
                block = x_ref[v * parts + part, unit * short : (unit + 1) * short]
                plain[unit * UNIT : (unit + 1) * UNIT, part * share : (part + 1) * share] = unpack(block, share)[:, 0:share]
        out_ref[0, :, v, :] = jnp.transpose(plain[...], (1, 0))


def finish(x, hemis, lats, levels, local, share):
    sectors, rows, _ = x.shape
    each = sectors // hemis
    return pl.pallas_call(
        functools.partial(finish_kernel, levels=levels, parts=each // levels, share=share),
        grid=(hemis,),
        in_specs=[pl.BlockSpec((each, rows, LANES), lambda h: (h, 0, 0))],
        out_specs=pl.BlockSpec((1, lats, levels, local), lambda h: (h, 0, 0, 0)),
        out_shape=jax.ShapeDtypeStruct((hemis, lats, levels, local), F32),
        scratch_shapes=[pltpu.VMEM((local, lats), F32)],
        compiler_params=params("arbitrary"),
        name="finish",
    )(x)


def transform(kernel, inputs, tables, out_rows, scratch_rows, **settings):
    matrix = tables[0]
    outs = tuple(jax.ShapeDtypeStruct((n, LANES), F32) for n in out_rows)
    return pl.pallas_call(
        functools.partial(kernel, **settings),
        out_shape=outs,
        scratch_shapes=[pltpu.VMEM((n, LANES), F32) for n in scratch_rows],
        compiler_params=pltpu.CompilerParams(vmem_limit_bytes=48 * 1024 * 1024),
        cost_estimate=cost(3 * 2 * matrix.size * LANES * settings["radix"], 8 * sum(out_rows) * LANES),
    )(*inputs, *tables)


def row_masks(pair, waves, shape, first):
    column = first + lax.broadcasted_iota(jnp.int32, shape, 1)
    limit = waves - pair
    leading = column < limit
    lag = jnp.where(leading, column, column - limit)
    odd = (lag & 1) == 1
    return column, leading, odd


def ranges(count):
    edges = list(range(0, count - count % WIDE, WIDE)) + [count]
    return list(zip(edges[:-1], edges[1:]))


def gather_lats(z_ref, hemi, level, levels, parts, share, start):
    rows = [z_ref[(hemi * levels + level) * parts + part, pl.ds(start, 8), 0:share] for part in range(parts)]
    return jnp.concatenate(rows, axis=1)


def legendre_stream(place_ref, legendre_ref, buffer, sems, step, steps):
    def copies(step, slot):
        pair = 2 * (place_ref[0] + step)
        return [
            pltpu.make_async_copy(legendre_ref.at[pair + n], buffer.at[slot, n], sems.at[slot, n]) for n in range(2)
        ]

    return stream(step, steps, DEPTH, copies)


def analyse_kernel(place_ref, z_ref, legendre_ref, out_ref, buffer, sems, *, levels, parts, share, steps):
    inner = out_ref.shape[0]
    count = legendre_ref.shape[2]
    waves = count - 1

    def body(index, carry):
        local_step = pl.program_id(0) * inner + index
        slot = legendre_stream(place_ref, legendre_ref, buffer, sems, local_step, steps)
        start = pl.multiple_of((place_ref[2] + local_step) * 8, 8)
        sums, differences = [], []
        for v in range(levels):
            north = gather_lats(z_ref, 0, v, levels, parts, share, start)
            south = gather_lats(z_ref, 1, v, levels, parts, share, start)
            sums.append(north + south)
            differences.append(north - south)
        stacks = []
        for which in range(2):
            low, high = which * 4, which * 4 + 4
            wave = jnp.concatenate([x[low:high] for x in sums + differences], axis=0)
            wave_high, wave_low = split(wave)
            stacks.append((jnp.concatenate([wave_high, wave_low], axis=0), wave_high))
        for first, last in ranges(count):
            picked = []
            for which in range(2):
                both, wave_high = stacks[which]
                rows = both.shape[0] // 2
                high, low = split(buffer[slot, which, :, first:last])
                product = jnp.dot(both, high, preferred_element_type=F32)
                product = product[0:rows] + product[rows:] + jnp.dot(wave_high, low, preferred_element_type=F32)
                pair = place_ref[1] + 2 * (place_ref[0] + local_step) + which
                shape = (rows // 2, last - first)
                _, leading, odd = row_masks(pair, waves, shape, first)
                chosen = jnp.where(odd, product[rows // 2 :], product[0 : rows // 2])
                if which == 0:
                    picked.append(jnp.where(leading, chosen, jnp.roll(chosen, -2, axis=0)))
                else:
                    picked.append(jnp.where(leading, jnp.roll(chosen, 2, axis=0), chosen))
            component = lax.broadcasted_iota(jnp.int32, picked[0].shape, 0) % 4
            out_ref[index, :, first:last] = jnp.where(component < 2, picked[0], picked[1])
        return carry

    lax.fori_loop(0, inner, body, 0)


def analyse(place, z, legendre, steps, levels):
    _, lats, count = legendre.shape
    parts = z.shape[0] // (2 * levels)
    share = lats // parts
    inner = math.gcd(steps, INNER)
    return pl.pallas_call(
        functools.partial(analyse_kernel, levels=levels, parts=parts, share=share, steps=steps),
        grid_spec=pltpu.PrefetchScalarGridSpec(
            num_scalar_prefetch=1,
            grid=(steps // inner,),
            in_specs=[
                pl.BlockSpec(z.shape, lambda i, place: (0, 0, 0)),
                pl.BlockSpec(memory_space=pl.ANY),
            ],
            out_specs=pl.BlockSpec((inner, 4 * levels, count), lambda i, place: (i, 0, 0)),
            scratch_shapes=[
                pltpu.VMEM((DEPTH, 2, lats, count), F32),
                pltpu.SemaphoreType.DMA((DEPTH, 2)),
            ],
        ),
        out_shape=jax.ShapeDtypeStruct((steps, 4 * levels, count), F32),
        compiler_params=params("arbitrary"),
        cost_estimate=cost(16 * 2 * steps * lats * count * WEIGHT, 2 * steps * lats * count * 4),
        name="analyse",
    )(place, z, legendre)


def synthesise_kernel(place_ref, damping_ref, spectrum_ref, legendre_ref, *rest, levels, parts, share, steps):
    out_ref, buffer, sems = rest[-3:]
    inner = spectrum_ref.shape[0]
    count = legendre_ref.shape[2]
    waves = count - 1

    def body(index, carry):
        local_step = pl.program_id(0) * inner + index
        step = place_ref[0] + local_step
        slot = legendre_stream(place_ref, legendre_ref, buffer, sems, local_step, steps)
        target = pl.multiple_of(index * 8, 8)
        totals = [None, None]
        for first, last in ranges(count):
            spectrum = spectrum_ref[index, :, first:last]
            row = lax.broadcasted_iota(jnp.int32, spectrum.shape, 0)
            component = row % 4
            damping = jnp.full(spectrum.shape, damping_ref[levels - 1])
            for v in range(levels - 1):
                damping = jnp.where(row < 4 * (v + 1), damping_ref[v], damping) if v == 0 else damping
            for which in range(2):
                pair = place_ref[1] + 2 * step + which
                column, leading, odd = row_masks(pair, waves, spectrum.shape, first)
                degree = jnp.where(leading, pair + column, column - 1)
                ratio = (degree * (degree + 1)).astype(F32) / float(waves * waves)
                solved = spectrum / (1.0 + damping * ratio)
                if which == 0:
                    doubled = jnp.where(component < 2, solved, jnp.roll(solved, 2, axis=0))
                else:
                    doubled = jnp.where(component < 2, jnp.roll(solved, -2, axis=0), solved)
                keep = jnp.logical_xor(component >= 2, leading)
                north = jnp.where(keep, doubled, 0.0)
                south = jnp.where(odd, -north, north)
                high, low = split(jnp.concatenate([north, south], axis=0))
                both = jnp.concatenate([high, low], axis=0)
                legendre_high, legendre_low = split(buffer[slot, which, :, first:last])
                contract = (((1,), (1,)), ((), ()))
                one = lax.dot_general(legendre_high, both, contract, preferred_element_type=F32)
                two = lax.dot_general(legendre_low, both, contract, preferred_element_type=F32)
                total = one + two
                totals[which] = total if totals[which] is None else totals[which] + total
        rows = 4 * levels * 2
        waves_of = []
        for which in range(2):
            turned = jnp.transpose(totals[which], (1, 0))
            waves_of.append(turned[0:rows] + turned[rows:])
        for hemi in range(2):
            for v in range(levels):
                low = (hemi * levels + v) * 4
                block = jnp.concatenate([w[low : low + 4] for w in waves_of], axis=0)
                for part in range(parts):
                    out_ref[(hemi * levels + v) * parts + part, pl.ds(target, 8), 0:share] = block[:, part * share : (part + 1) * share]
        return carry

    lax.fori_loop(0, inner, body, 0)


def synthesise(place, damping, spectrum, legendre, previous, sectors, rows):
    _, lats, count = legendre.shape
    levels = damping.shape[0]
    steps = spectrum.shape[0]
    parts = sectors // (2 * levels)
    share = lats // parts
    inner = math.gcd(steps, INNER)
    arguments = [place, damping, spectrum, legendre]
    in_specs = [
        pl.BlockSpec(memory_space=pltpu.SMEM),
        pl.BlockSpec((inner, 4 * levels, count), lambda i, place: (i, 0, 0)),
        pl.BlockSpec(memory_space=pl.ANY),
    ]
    aliases = {}
    if previous is not None:
        arguments.append(previous)
        in_specs.append(pl.BlockSpec(memory_space=pl.ANY))
        aliases = {4: 0}
    return pl.pallas_call(
        functools.partial(synthesise_kernel, levels=levels, parts=parts, share=share, steps=steps),
        grid_spec=pltpu.PrefetchScalarGridSpec(
            num_scalar_prefetch=1,
            grid=(steps // inner,),
            in_specs=in_specs,
            out_specs=pl.BlockSpec((sectors, 8 * inner, LANES), lambda i, place: (0, place[3] + i, 0)),
            scratch_shapes=[
                pltpu.VMEM((DEPTH, 2, lats, count), F32),
                pltpu.SemaphoreType.DMA((DEPTH, 2)),
            ],
        ),
        out_shape=jax.ShapeDtypeStruct((sectors, rows, LANES), F32),
        input_output_aliases=aliases,
        compiler_params=params("arbitrary"),
        cost_estimate=cost(16 * 2 * steps * lats * count * WEIGHT, 2 * steps * lats * count * 4),
        name="synthesise",
    )(*arguments)


def after(value, earlier):
    return value if earlier is None else lax.optimization_barrier((value, earlier))[0]


def exchange(x, sectors):
    return lax.all_to_all(x.reshape(sectors, -1, LANES), "sector", split_axis=0, concat_axis=0, tiled=True)


def solve(fourier, legendre, damping, sectors):
    pairs = legendre.shape[0]
    bands = lax.axis_size("band")
    levels = damping.shape[0]
    bit = lax.axis_index("band") % 2
    pair_start = lax.axis_index("sector") * pairs
    chunks = math.gcd(pairs // 4, CHUNKS)
    each = chunks // SPLITS
    steps = pairs // (2 * 2 * chunks)
    half = pairs // 4
    blocks = steps // math.gcd(steps, INNER)
    rows = 4 * pairs // SPLITS

    def place(side, chunk):
        inside = side * each + chunk % each
        return jnp.stack([side * half + chunk * steps, pair_start, inside * steps, inside * blocks]).astype(jnp.int32)

    def swap(x, mask):
        return lax.ppermute(x, "band", [(i, i ^ mask) for i in range(bands)])

    masks = [1 << n for n in range(1, bands.bit_length()) if 1 << n < bands]
    sums, arrived, z, kept = [], [], None, None
    for c in range(chunks):
        if c % each == 0:
            z = exchange(after(fourier[c // each], z), sectors)
        spot = after(place(1 - bit, c), kept)
        away = analyse(after(spot, sums[c - 2] if c >= 2 else None), z, legendre, steps, levels)
        kept = analyse(after(place(bit, c), away), z, legendre, steps, levels)
        sums.append(kept + swap(away, 1))
        arrived.append(swap(sums[c], masks[0]) if masks else jnp.zeros_like(kept))

    def finished(c, gate):
        total = sums[c] + after(arrived[c], gate)
        for mask in masks[1:]:
            total = total + swap(total, mask)
        return total, swap(total, 1)

    results, result = [], None
    total, other = finished(0, kept)
    for c in range(chunks):
        fresh = c % each == 0
        spot = after(place(bit, c), result) if fresh else place(bit, c)
        result = synthesise(spot, damping, total, legendre, None if fresh else result, sectors, rows)
        mine = other
        if c + 1 < chunks:
            total, other = finished(c + 1, result)
        result = synthesise(place(1 - bit, c), damping, mine, legendre, result, sectors, rows)
        if (c + 1) % each == 0:
            results.append(exchange(result, sectors))
    return results


def local(field, depart, interp_weight, legendre, damping):
    sectors = lax.axis_size("sector")
    hemis, lats, levels, local_lon = field.shape
    pairs = legendre.shape[0]
    lon_count = sectors * local_lon
    radix = math.gcd(RADIX, pairs)
    matrix, twiddle = fourier_tables(lon_count, radix)
    twiddle = jnp.broadcast_to(jnp.asarray(twiddle)[..., None], twiddle.shape + (LANES,))
    forward_tables = split_np(matrix / lon_count) + (twiddle,)
    inverse_tables = split_np(2.0 * matrix.T) + (twiddle,)
    sizes = dict(radix=radix, rows=lon_count, sectors=sectors)
    chunks = (lon_count // SPLITS,) * SPLITS

    advected, packed, share = advect(field, depart, interp_weight, sectors)
    columns = exchange(advected, sectors).reshape(-1, LANES)
    scratch = (lon_count, lon_count) if packed else (lon_count,)
    fourier = transform(forward_kernel, [columns], forward_tables, chunks, scratch, share=share, **sizes)
    returned = solve(fourier, legendre, damping, sectors)
    returned = [x.reshape(-1, LANES) for x in returned]
    final_rows = packed_rows(lon_count, share) if packed else lon_count
    gridded = transform(inverse_kernel, returned, inverse_tables, (final_rows,), scratch, share=share, **sizes)
    final = exchange(gridded[0], sectors)
    if packed:
        return finish(final, hemis, lats, levels, local_lon, share)
    parts = sectors // (hemis * levels)
    final = final[:, :, :share].reshape(hemis, levels, parts, local_lon, share)
    return jnp.transpose(final, (0, 2, 4, 1, 3)).reshape(hemis, lats, levels, local_lon)


def solution(mesh):
    return jax.shard_map(
        local,
        mesh=mesh,
        in_specs=(
            P(None, "band", None, "sector"),
            P(None, "band", "sector"),
            P(None, "band", "sector", None, None),
            P("sector", "band", None),
            P(),
        ),
        out_specs=P(None, "band", None, "sector"),
        check_vma=False,
    )
```

```python
import functools
import math

import jax
import jax.numpy as jnp
import numpy as np
from jax import lax
from jax.experimental import pallas as pl
from jax.experimental.pallas import tpu as pltpu
from jax.sharding import PartitionSpec as P


REACH_BACK = 2
REACH_AHEAD = 3
CHUNKS = 2
SPLITS = 2
INNER = 5
LANES = 128
UNIT = 64
RADIX = 16
DEPTH = 6
WEIGHT = 2
WIDE = 256
F32 = jnp.float32
BF16 = jnp.bfloat16


def params(*semantics):
    return pltpu.CompilerParams(dimension_semantics=semantics, vmem_limit_bytes=48 * 1024 * 1024)


def cost(flops, moved):
    return pl.CostEstimate(flops=int(flops), bytes_accessed=int(moved), transcendentals=0)


def split(x):
    high = x.astype(BF16)
    low = (x - high.astype(F32)).astype(BF16)
    return high, low


def split_np(x):
    high = np.asarray(x, np.float32).astype(jnp.bfloat16)
    low = (np.asarray(x, np.float64) - high.astype(np.float64)).astype(np.float32).astype(jnp.bfloat16)
    return high, low


def stream(step, steps, depth, copies):
    ahead = depth - 1

    @pl.when(step == 0)
    def _():
        for early in range(min(ahead, steps)):
            for copy in copies(early, early):
                copy.start()

    @pl.when(step + ahead < steps)
    def _():
        for copy in copies(step + ahead, lax.rem(step + ahead, depth)):
            copy.start()

    slot = lax.rem(step, depth)
    for copy in copies(step, slot):
        copy.wait()
    return slot


def piece_widths(share):
    return [w for w in (64, 32, 16) if share & w]


def packable(share, rows, lanes=LANES):
    return share < lanes and share % 16 == 0 and rows % UNIT == 0


def packed_rows(rows, share):
    return rows * share // LANES


def pack(x, share):
    rows, offset, blocks = x.shape[0], 0, []
    for w in piece_widths(share):
        folds = LANES // w
        h = rows // folds
        blocks.append(jnp.concatenate([x[b * h : (b + 1) * h, offset : offset + w] for b in range(folds)], axis=1))
        offset += w
    return jnp.concatenate(blocks, axis=0)


def unpack(y, share):
    rows = y.shape[0] * LANES // share
    first, columns = 0, []
    for w in piece_widths(share):
        folds = LANES // w
        h = rows // folds
        block = y[first : first + h]
        columns.append(jnp.concatenate([block[:, b * w : (b + 1) * w] for b in range(folds)], axis=0))
        first += h
    columns.append(jnp.zeros((rows, LANES - share), y.dtype))
    return jnp.concatenate(columns, axis=1)


def advect_kernel(groups_ref, *refs, width, parts, share, group, count, packed, halo):
    if halo:
        field_ref, before_ref, after_ref, depart_ref, weight_ref, _, out_ref, extended, window, weights, sems = refs
    else:
        field_ref, depart_ref, weight_ref, out_ref, extended, window, weights, sems = refs
    hemi, place = pl.program_id(0), pl.program_id(1)
    levels, local, columns = field_ref.shape[1], field_ref.shape[2], field_ref.shape[3]
    back, ahead = REACH_BACK * width, REACH_AHEAD * width

    @pl.when(place == 0)
    def _():
        for v in range(levels):
            extended[v, back : back + local] = field_ref[0, v]
            if halo:
                extended[v, 0:back] = before_ref[0, v]
                extended[v, back + local : back + local + ahead] = after_ref[0, v]

    def copies(step, slot):
        tiles = groups_ref[lax.rem(step, count)] * group
        source = lax.div(step, count)
        return [
            pltpu.make_async_copy(weight_ref.at[source, tiles + n], weights.at[slot, n], sems.at[slot, n])
            for n in range(group)
        ]

    slot = stream(hemi * count + place, 2 * count, DEPTH, copies)
    results = [[] for _ in range(levels)]
    for n in range(group):
        tile = groups_ref[place] * group + n
        depart = depart_ref[0, n]
        start = pl.multiple_of(tile * width, width)
        for v in range(levels):
            for half in range(0, 2 * width, 8):
                picked = None
                for step in range(2 * REACH_BACK + 1):
                    rows = extended[v, pl.ds(start + step * width + half, 8), :]
                    chosen = depart == (step - REACH_BACK)
                    picked = rows if picked is None else jnp.where(chosen, rows, picked)
                window[v, half : half + 8] = picked

        def body(block, totals):
            for j in range(8):
                row = block * 8 + j
                weight = weights[slot, n, row].astype(F32)
                totals = tuple(totals[v] + window[v, pl.ds(row, 1), :] * weight for v in range(levels))
            return totals

        zero = jnp.zeros((width, columns), F32)
        totals = lax.fori_loop(0, 2 * width // 8, body, (zero,) * levels)
        for v in range(levels):
            results[v].append(totals[v])
    for v in range(levels):
        value = jnp.concatenate(results[v], axis=0)
        for part in range(parts):
            mine = value[:, part * share : (part + 1) * share]
            if packed:
                out_ref[v * parts + part] = pack(mine, share)
            else:
                out_ref[v * parts + part, :, 0:share] = mine


def advect(field, depart, interp_weight, sectors):
    hemis, lats, levels, local = field.shape
    width = interp_weight.shape[-1]
    tiles = depart.shape[2]
    parts = sectors // (hemis * levels)
    share = lats // parts
    packed = packable(share, local) and UNIT % width == 0
    group = UNIT // width if packed else 1
    rows = packed_rows(group * width, share) if packed else width
    turned = jnp.transpose(field, (0, 2, 3, 1))
    up = [(i, (i + 1) % sectors) for i in range(sectors)]
    down = [(j, i) for i, j in up]
    before = lax.ppermute(turned[:, :, local - REACH_BACK * width :], "sector", up)
    after = lax.ppermute(turned[:, :, : REACH_AHEAD * width], "sector", down)
    weights = jnp.transpose(interp_weight, (0, 2, 3, 4, 1))
    offsets = jnp.transpose(depart, (0, 2, 1))[:, :, None, :]
    every = list(range(tiles // group))
    inner = [g for g in every if g * group >= REACH_BACK and (g + 1) * group - 1 + REACH_AHEAD < tiles]
    outer = [g for g in every if g not in inner]

    def call(groups, halo, previous):
        count = len(groups)
        field_specs = [pl.BlockSpec((1, levels, local, lats), lambda h, g, groups: (h, 0, 0, 0))]
        operands = [jnp.asarray(groups, jnp.int32), turned]
        if halo:
            for side in (before, after):
                field_specs.append(pl.BlockSpec((1,) + side.shape[1:], lambda h, g, groups: (h, 0, 0, 0)))
                operands.append(side)
        operands += [offsets, weights]
        in_specs = field_specs + [
            pl.BlockSpec((1, group, 1, lats), lambda h, g, groups: (h, groups[g], 0, 0)),
            pl.BlockSpec(memory_space=pl.ANY),
        ]
        aliases = {}
        if halo:
            operands.append(previous)
            in_specs.append(pl.BlockSpec(memory_space=pl.ANY))
            aliases = {len(operands) - 1: 0}
        return pl.pallas_call(
            functools.partial(advect_kernel, width=width, parts=parts, share=share, group=group, count=count, packed=packed, halo=halo),
            grid_spec=pltpu.PrefetchScalarGridSpec(
                num_scalar_prefetch=1,
                grid=(hemis, count),
                in_specs=in_specs,
                out_specs=pl.BlockSpec((levels * parts, rows, LANES), lambda h, g, groups: (h, groups[g], 0)),
                scratch_shapes=[
                    pltpu.VMEM((levels, local + (REACH_BACK + REACH_AHEAD) * width, lats), F32),
                    pltpu.VMEM((levels, 2 * width, lats), F32),
                    pltpu.VMEM((DEPTH, group, 2 * width, width, lats), BF16),
                    pltpu.SemaphoreType.DMA((DEPTH, group)),
                ],
            ),
            out_shape=jax.ShapeDtypeStruct((sectors, rows * len(every), LANES), F32),
            input_output_aliases=aliases,
            compiler_params=params("arbitrary", "arbitrary"),
            cost_estimate=cost(4 * hemis * count * group * levels * 2 * width * width * lats * 4, interp_weight.size * 3 * count // len(every)),
            name="advect_edge" if halo else "advect_inner",
        )(*operands)

    if inner:
        result = call(inner, False, None)
    else:
        result = jnp.zeros((sectors, rows * len(every), LANES), F32)
    return call(outer, True, result), packed, share


def fourier_tables(lon_count, radix):
    inner = lon_count // radix
    waves = lon_count // 2
    slots = waves // 2 // radix
    index = np.arange(slots)
    direct = index
    mirror = waves // radix - 1 - index
    rows = []
    for kind in range(2):
        for component in range(4):
            degree = direct if component < 2 else mirror
            source = degree if kind == 0 else inner - 1 - degree
            angle = 2.0 * np.pi * ((source[:, None] * np.arange(inner)[None, :]) % inner) / inner
            if component % 2 == 0:
                row = np.concatenate([np.cos(angle), np.sin(angle)], axis=1)
            else:
                sign = 1.0 if kind == 0 else -1.0
                row = sign * np.concatenate([-np.sin(angle), np.cos(angle)], axis=1)
            rows.append(row)
    matrix = np.concatenate(rows, axis=0)
    order = np.arange(radix // 2 + 1)[:, None] * np.arange(inner)[None, :]
    angle = 2.0 * np.pi * (order % lon_count) / lon_count
    twiddle = np.stack([np.cos(angle), -np.sin(angle)], axis=1).astype(np.float32)
    return matrix, twiddle


def scaled(x, factor):
    if abs(factor - 1.0) < 1e-12:
        return x
    if abs(factor + 1.0) < 1e-12:
        return -x
    return x * np.float32(factor)


def combine(terms):
    total = None
    for factor, x in terms:
        if abs(factor) < 1e-12:
            continue
        total = scaled(x, factor) if total is None else total + scaled(x, factor)
    return total


def products(high_ref, low_ref, rows, depth, x):
    x_high, x_low = split(x)
    both = jnp.concatenate([x_high, x_low], axis=1)
    first = jnp.dot(high_ref[0:rows, 0:depth], both, preferred_element_type=F32)
    second = jnp.dot(low_ref[0:rows, 0:depth], x_high, preferred_element_type=F32)
    return first[:, 0:LANES] + first[:, LANES:] + second


def places(a, radix):
    residues = [a] if a in (0, radix // 2) else [a, radix - a]
    result = []
    for residue in residues:
        for component in range(4):
            first = residue if component < 2 else radix - 1 - residue
            result.append(first * 4 + component)
    return result


def chunk_rows(rows, sectors):
    n = rows // (sectors * 2 * SPLITS)
    return [(block * n, block * n * SPLITS, n) for block in range(sectors * 2)]


def forward_kernel(x_ref, high_ref, low_ref, twiddle_ref, *refs, radix, share, rows, sectors):
    outs, scratch = refs[:SPLITS], refs[SPLITS:]
    inner = rows // radix
    slots = rows // (4 * radix)
    out_ref = scratch[0]
    if len(scratch) > 1:
        plain = scratch[1]
        short = packed_rows(UNIT, share)
        for unit in range(rows // UNIT):
            plain[unit * UNIT : (unit + 1) * UNIT] = unpack(x_ref[unit * short : (unit + 1) * short], share)
    else:
        plain = x_ref
    x = [plain[s * inner : (s + 1) * inner] for s in range(radix)]
    middle = radix // 2
    even = {s: x[s] + x[radix - s] for s in range(1, middle)}
    odd = {s: x[s] - x[radix - s] for s in range(1, middle)}
    for a in range(middle + 1):
        angle = [2.0 * math.pi * ((a * s) % radix) / radix for s in range(radix)]
        real = combine([(1.0, x[0]), (math.cos(angle[middle]), x[middle])] + [(math.cos(angle[s]), even[s]) for s in even])
        imag = combine([(-math.sin(angle[s]), odd[s]) for s in odd])
        where = places(a, radix)
        if a == 0:
            result = products(high_ref, low_ref, len(where) * slots, inner, real)
        else:
            cos, sin = twiddle_ref[a, 0], twiddle_ref[a, 1]
            turned_real = cos * real if imag is None else cos * real - sin * imag
            turned_imag = sin * real if imag is None else sin * real + cos * imag
            turned = jnp.concatenate([turned_real, turned_imag], axis=0)
            result = products(high_ref, low_ref, len(where) * slots, 2 * inner, turned)
        for n, first in enumerate(where):
            out_ref[pl.ds(first, slots, stride=4 * radix), :] = result[n * slots : (n + 1) * slots]
    for target, source, n in chunk_rows(rows, sectors):
        for c in range(SPLITS):
            outs[c][target : target + n] = out_ref[source + c * n : source + (c + 1) * n]


def inverse_kernel(*refs, radix, share, rows, sectors):
    ins, (high_ref, low_ref, twiddle_ref, final_ref, z_ref, *scratch) = refs[:SPLITS], refs[SPLITS:]
    out_ref = scratch[0] if scratch else final_ref
    inner = rows // radix
    slots = rows // (4 * radix)
    for source, target, n in chunk_rows(rows, sectors):
        for c in range(SPLITS):
            z_ref[target + c * n : target + (c + 1) * n] = ins[c][source : source + n]
    middle = radix // 2
    reals, imags = [], []
    for a in range(middle + 1):
        where = places(a, radix)
        pieces = [z_ref[pl.ds(first, slots, stride=4 * radix), :] for first in where]
        if a == 0:
            row = lax.broadcasted_iota(jnp.int32, pieces[0].shape, 0)
            pieces[0] = jnp.where(row == 0, 0.5 * pieces[0], pieces[0])
        column = jnp.concatenate(pieces, axis=0)
        depth = len(where) * slots
        if a == 0:
            reals.append(products(high_ref, low_ref, inner, depth, column))
            imags.append(None)
            continue
        result = products(high_ref, low_ref, 2 * inner, depth, column)
        real, imag = result[0:inner], result[inner:]
        cos, sin = twiddle_ref[a, 0], twiddle_ref[a, 1]
        reals.append(cos * real + sin * imag)
        imags.append(None if a == middle else cos * imag - sin * real)
    for s in range(middle + 1):
        angle = [2.0 * math.pi * ((a * s) % radix) / radix for a in range(middle + 1)]
        even = combine([(math.cos(angle[a]), reals[a]) for a in range(middle + 1)])
        odd = combine([(-math.sin(angle[a]), imags[a]) for a in range(1, middle)])
        if s == 0 or s == middle:
            out_ref[s * inner : (s + 1) * inner] = even
        else:
            out_ref[s * inner : (s + 1) * inner] = even + odd
            other = radix - s
            out_ref[other * inner : (other + 1) * inner] = even - odd
    if scratch:
        short = packed_rows(UNIT, share)
        for unit in range(rows // UNIT):
            final_ref[unit * short : (unit + 1) * short] = pack(out_ref[unit * UNIT : (unit + 1) * UNIT], share)


def finish_kernel(x_ref, out_ref, plain, *, levels, parts, share):
    short = packed_rows(UNIT, share)
    for v in range(levels):
        for part in range(parts):
            for unit in range(plain.shape[0] // UNIT):
                block = x_ref[v * parts + part, unit * short : (unit + 1) * short]
                plain[unit * UNIT : (unit + 1) * UNIT, part * share : (part + 1) * share] = unpack(block, share)[:, 0:share]
        out_ref[0, :, v, :] = jnp.transpose(plain[...], (1, 0))


def finish(x, hemis, lats, levels, local, share):
    sectors, rows, _ = x.shape
    each = sectors // hemis
    return pl.pallas_call(
        functools.partial(finish_kernel, levels=levels, parts=each // levels, share=share),
        grid=(hemis,),
        in_specs=[pl.BlockSpec((each, rows, LANES), lambda h: (h, 0, 0))],
        out_specs=pl.BlockSpec((1, lats, levels, local), lambda h: (h, 0, 0, 0)),
        out_shape=jax.ShapeDtypeStruct((hemis, lats, levels, local), F32),
        scratch_shapes=[pltpu.VMEM((local, lats), F32)],
        compiler_params=params("arbitrary"),
        name="finish",
    )(x)


def transform(kernel, inputs, tables, out_rows, scratch_rows, **settings):
    matrix = tables[0]
    outs = tuple(jax.ShapeDtypeStruct((n, LANES), F32) for n in out_rows)
    return pl.pallas_call(
        functools.partial(kernel, **settings),
        out_shape=outs,
        scratch_shapes=[pltpu.VMEM((n, LANES), F32) for n in scratch_rows],
        compiler_params=pltpu.CompilerParams(vmem_limit_bytes=48 * 1024 * 1024),
        cost_estimate=cost(3 * 2 * matrix.size * LANES * settings["radix"], 8 * sum(out_rows) * LANES),
    )(*inputs, *tables)


def row_masks(pair, waves, shape, first):
    column = first + lax.broadcasted_iota(jnp.int32, shape, 1)
    limit = waves - pair
    leading = column < limit
    lag = jnp.where(leading, column, column - limit)
    odd = (lag & 1) == 1
    return column, leading, odd


def ranges(count):
    edges = list(range(0, count - count % WIDE, WIDE)) + [count]
    return list(zip(edges[:-1], edges[1:]))


def gather_lats(z_ref, hemi, level, levels, parts, share, start):
    rows = [z_ref[(hemi * levels + level) * parts + part, pl.ds(start, 8), 0:share] for part in range(parts)]
    return jnp.concatenate(rows, axis=1)


def legendre_stream(place_ref, legendre_ref, buffer, sems, step, steps):
    def copies(step, slot):
        pair = 2 * (place_ref[0] + step)
        return [
            pltpu.make_async_copy(legendre_ref.at[pair + n], buffer.at[slot, n], sems.at[slot, n]) for n in range(2)
        ]

    return stream(step, steps, DEPTH, copies)


def analyse_kernel(place_ref, z_ref, legendre_ref, out_ref, buffer, sems, *, levels, parts, share, steps):
    inner = out_ref.shape[0]
    count = legendre_ref.shape[2]
    waves = count - 1

    def body(index, carry):
        local_step = pl.program_id(0) * inner + index
        slot = legendre_stream(place_ref, legendre_ref, buffer, sems, local_step, steps)
        start = pl.multiple_of((place_ref[2] + local_step) * 8, 8)
        sums, differences = [], []
        for v in range(levels):
            north = gather_lats(z_ref, 0, v, levels, parts, share, start)
            south = gather_lats(z_ref, 1, v, levels, parts, share, start)
            sums.append(north + south)
            differences.append(north - south)
        stacks = []
        for which in range(2):
            low, high = which * 4, which * 4 + 4
            wave = jnp.concatenate([x[low:high] for x in sums + differences], axis=0)
            wave_high, wave_low = split(wave)
            stacks.append((jnp.concatenate([wave_high, wave_low], axis=0), wave_high))
        for first, last in ranges(count):
            picked = []
            for which in range(2):
                both, wave_high = stacks[which]
                rows = both.shape[0] // 2
                high, low = split(buffer[slot, which, :, first:last])
                product = jnp.dot(both, high, preferred_element_type=F32)
                product = product[0:rows] + product[rows:] + jnp.dot(wave_high, low, preferred_element_type=F32)
                pair = place_ref[1] + 2 * (place_ref[0] + local_step) + which
                shape = (rows // 2, last - first)
                _, leading, odd = row_masks(pair, waves, shape, first)
                chosen = jnp.where(odd, product[rows // 2 :], product[0 : rows // 2])
                if which == 0:
                    picked.append(jnp.where(leading, chosen, jnp.roll(chosen, -2, axis=0)))
                else:
                    picked.append(jnp.where(leading, jnp.roll(chosen, 2, axis=0), chosen))
            component = lax.broadcasted_iota(jnp.int32, picked[0].shape, 0) % 4
            out_ref[index, :, first:last] = jnp.where(component < 2, picked[0], picked[1])
        return carry

    lax.fori_loop(0, inner, body, 0)


def analyse(place, z, legendre, steps, levels):
    _, lats, count = legendre.shape
    parts = z.shape[0] // (2 * levels)
    share = lats // parts
    inner = math.gcd(steps, INNER)
    return pl.pallas_call(
        functools.partial(analyse_kernel, levels=levels, parts=parts, share=share, steps=steps),
        grid_spec=pltpu.PrefetchScalarGridSpec(
            num_scalar_prefetch=1,
            grid=(steps // inner,),
            in_specs=[
                pl.BlockSpec(z.shape, lambda i, place: (0, 0, 0)),
                pl.BlockSpec(memory_space=pl.ANY),
            ],
            out_specs=pl.BlockSpec((inner, 4 * levels, count), lambda i, place: (i, 0, 0)),
            scratch_shapes=[
                pltpu.VMEM((DEPTH, 2, lats, count), F32),
                pltpu.SemaphoreType.DMA((DEPTH, 2)),
            ],
        ),
        out_shape=jax.ShapeDtypeStruct((steps, 4 * levels, count), F32),
        compiler_params=params("arbitrary"),
        cost_estimate=cost(16 * 2 * steps * lats * count * WEIGHT, 2 * steps * lats * count * 4),
        name="analyse",
    )(place, z, legendre)


def synthesise_kernel(place_ref, damping_ref, spectrum_ref, legendre_ref, *rest, levels, parts, share, steps):
    out_ref, buffer, sems = rest[-3:]
    inner = spectrum_ref.shape[0]
    count = legendre_ref.shape[2]
    waves = count - 1

    def body(index, carry):
        local_step = pl.program_id(0) * inner + index
        step = place_ref[0] + local_step
        slot = legendre_stream(place_ref, legendre_ref, buffer, sems, local_step, steps)
        target = pl.multiple_of(index * 8, 8)
        totals = [None, None]
        for first, last in ranges(count):
            spectrum = spectrum_ref[index, :, first:last]
            row = lax.broadcasted_iota(jnp.int32, spectrum.shape, 0)
            component = row % 4
            damping = jnp.full(spectrum.shape, damping_ref[levels - 1])
            for v in range(levels - 1):
                damping = jnp.where(row < 4 * (v + 1), damping_ref[v], damping) if v == 0 else damping
            for which in range(2):
                pair = place_ref[1] + 2 * step + which
                column, leading, odd = row_masks(pair, waves, spectrum.shape, first)
                degree = jnp.where(leading, pair + column, column - 1)
                ratio = (degree * (degree + 1)).astype(F32) / float(waves * waves)
                solved = spectrum / (1.0 + damping * ratio)
                if which == 0:
                    doubled = jnp.where(component < 2, solved, jnp.roll(solved, 2, axis=0))
                else:
                    doubled = jnp.where(component < 2, jnp.roll(solved, -2, axis=0), solved)
                keep = jnp.logical_xor(component >= 2, leading)
                north = jnp.where(keep, doubled, 0.0)
                south = jnp.where(odd, -north, north)
                high, low = split(jnp.concatenate([north, south], axis=0))
                both = jnp.concatenate([high, low], axis=0)
                legendre_high, legendre_low = split(buffer[slot, which, :, first:last])
                contract = (((1,), (1,)), ((), ()))
                one = lax.dot_general(legendre_high, both, contract, preferred_element_type=F32)
                two = lax.dot_general(legendre_low, both, contract, preferred_element_type=F32)
                total = one + two
                totals[which] = total if totals[which] is None else totals[which] + total
        rows = 4 * levels * 2
        waves_of = []
        for which in range(2):
            turned = jnp.transpose(totals[which], (1, 0))
            waves_of.append(turned[0:rows] + turned[rows:])
        for hemi in range(2):
            for v in range(levels):
                low = (hemi * levels + v) * 4
                block = jnp.concatenate([w[low : low + 4] for w in waves_of], axis=0)
                for part in range(parts):
                    out_ref[(hemi * levels + v) * parts + part, pl.ds(target, 8), 0:share] = block[:, part * share : (part + 1) * share]
        return carry

    lax.fori_loop(0, inner, body, 0)


def synthesise(place, damping, spectrum, legendre, previous, sectors, rows):
    _, lats, count = legendre.shape
    levels = damping.shape[0]
    steps = spectrum.shape[0]
    parts = sectors // (2 * levels)
    share = lats // parts
    inner = math.gcd(steps, INNER)
    arguments = [place, damping, spectrum, legendre]
    in_specs = [
        pl.BlockSpec(memory_space=pltpu.SMEM),
        pl.BlockSpec((inner, 4 * levels, count), lambda i, place: (i, 0, 0)),
        pl.BlockSpec(memory_space=pl.ANY),
    ]
    aliases = {}
    if previous is not None:
        arguments.append(previous)
        in_specs.append(pl.BlockSpec(memory_space=pl.ANY))
        aliases = {4: 0}
    return pl.pallas_call(
        functools.partial(synthesise_kernel, levels=levels, parts=parts, share=share, steps=steps),
        grid_spec=pltpu.PrefetchScalarGridSpec(
            num_scalar_prefetch=1,
            grid=(steps // inner,),
            in_specs=in_specs,
            out_specs=pl.BlockSpec((sectors, 8 * inner, LANES), lambda i, place: (0, place[3] + i, 0)),
            scratch_shapes=[
                pltpu.VMEM((DEPTH, 2, lats, count), F32),
                pltpu.SemaphoreType.DMA((DEPTH, 2)),
            ],
        ),
        out_shape=jax.ShapeDtypeStruct((sectors, rows, LANES), F32),
        input_output_aliases=aliases,
        compiler_params=params("arbitrary"),
        cost_estimate=cost(16 * 2 * steps * lats * count * WEIGHT, 2 * steps * lats * count * 4),
        name="synthesise",
    )(*arguments)


def after(value, earlier):
    return value if earlier is None else lax.optimization_barrier((value, earlier))[0]


def exchange(x, sectors):
    return lax.all_to_all(x.reshape(sectors, -1, LANES), "sector", split_axis=0, concat_axis=0, tiled=True)


def solve(fourier, legendre, damping, sectors):
    pairs = legendre.shape[0]
    bands = lax.axis_size("band")
    levels = damping.shape[0]
    bit = lax.axis_index("band") % 2
    pair_start = lax.axis_index("sector") * pairs
    chunks = math.gcd(pairs // 4, CHUNKS)
    each = chunks // SPLITS
    steps = pairs // (2 * 2 * chunks)
    half = pairs // 4
    blocks = steps // math.gcd(steps, INNER)
    rows = 4 * pairs // SPLITS

    def place(side, chunk):
        inside = side * each + chunk % each
        return jnp.stack([side * half + chunk * steps, pair_start, inside * steps, inside * blocks]).astype(jnp.int32)

    def swap(x, mask):
        return lax.ppermute(x, "band", [(i, i ^ mask) for i in range(bands)])

    masks = [1 << n for n in range(1, bands.bit_length()) if 1 << n < bands]
    sums, arrived, z, kept = [], [], None, None
    for c in range(chunks):
        if c % each == 0:
            z = exchange(after(fourier[c // each], z), sectors)
        spot = after(place(1 - bit, c), kept)
        away = analyse(after(spot, sums[c - 2] if c >= 2 else None), z, legendre, steps, levels)
        kept = analyse(after(place(bit, c), away), z, legendre, steps, levels)
        sums.append(kept + swap(away, 1))
        arrived.append(swap(sums[c], masks[0]) if masks else jnp.zeros_like(kept))

    def finished(c, gate):
        total = sums[c] + after(arrived[c], gate)
        for mask in masks[1:]:
            total = total + swap(total, mask)
        return total, swap(total, 1)

    results, result = [], None
    total, other = finished(0, kept)
    for c in range(chunks):
        fresh = c % each == 0
        spot = after(place(bit, c), result) if fresh else place(bit, c)
        result = synthesise(spot, damping, total, legendre, None if fresh else result, sectors, rows)
        result = synthesise(place(1 - bit, c), damping, other, legendre, result, sectors, rows)
        if c + 1 < chunks:
            total, other = finished(c + 1, result)
        if (c + 1) % each == 0:
            results.append(exchange(result, sectors))
    return results


def local(field, depart, interp_weight, legendre, damping):
    sectors = lax.axis_size("sector")
    hemis, lats, levels, local_lon = field.shape
    pairs = legendre.shape[0]
    lon_count = sectors * local_lon
    radix = math.gcd(RADIX, pairs)
    matrix, twiddle = fourier_tables(lon_count, radix)
    twiddle = jnp.broadcast_to(jnp.asarray(twiddle)[..., None], twiddle.shape + (LANES,))
    forward_tables = split_np(matrix / lon_count) + (twiddle,)
    inverse_tables = split_np(2.0 * matrix.T) + (twiddle,)
    sizes = dict(radix=radix, rows=lon_count, sectors=sectors)
    chunks = (lon_count // SPLITS,) * SPLITS

    advected, packed, share = advect(field, depart, interp_weight, sectors)
    columns = exchange(advected, sectors).reshape(-1, LANES)
    scratch = (lon_count, lon_count) if packed else (lon_count,)
    fourier = transform(forward_kernel, [columns], forward_tables, chunks, scratch, share=share, **sizes)
    returned = solve(fourier, legendre, damping, sectors)
    returned = [x.reshape(-1, LANES) for x in returned]
    final_rows = packed_rows(lon_count, share) if packed else lon_count
    gridded = transform(inverse_kernel, returned, inverse_tables, (final_rows,), scratch, share=share, **sizes)
    final = exchange(gridded[0], sectors)
    if packed:
        return finish(final, hemis, lats, levels, local_lon, share)
    parts = sectors // (hemis * levels)
    final = final[:, :, :share].reshape(hemis, levels, parts, local_lon, share)
    return jnp.transpose(final, (0, 2, 4, 1, 3)).reshape(hemis, lats, levels, local_lon)


def solution(mesh):
    return jax.shard_map(
        local,
        mesh=mesh,
        in_specs=(
            P(None, "band", None, "sector"),
            P(None, "band", "sector"),
            P(None, "band", "sector", None, None),
            P("sector", "band", None),
            P(),
        ),
        out_specs=P(None, "band", None, "sector"),
        check_vma=False,
    )
```
